32 devices in a mesh: gz: 8 (over z, x), col: 4 (over y, core).
Axes of the slice: x: 2, y: 2, z: 4, core: 2. Of those that a mesh axis runs over, the one named last changes fastest.
Arguments:
- source: float32 [512, 2048], P('gz', 'col'), may hold values from -6 to 6
- z_vectors: float32 [512, 512], P('gz', 'col'), may hold values from -0.375 to 0.375
- x_vectors: float32 [4, 4], replicated, may hold values from -3 to 3
- y_vectors: float32 [512, 512], replicated, may hold values from -0.25 to 0.25
- z_values: float32 [512], replicated, may hold values from 0.1 to 3
- x_values: float32 [4], replicated, may hold values from 0.1 to 3
- y_values: float32 [512], replicated, may hold values from 0.1 to 3
Outputs:
- solution: float32 [512, 2048], P('gz', 'col')
The draws below stay inside these ranges and needn't reach their ends.
All inputs are finite; a program needn't handle non-finite values.
Results may differ from the reference program's by a relative error of at most 0.000092.
Values sent between devices are 32-bit elements; how exact they have to be, the bound alone decides.
A program may use at most 64 MiB of HBM per device.

```python
import math
import jax
import jax.numpy as jnp
from jax import lax

NY = 512
NZ = 512
NX = 4


def strengthened(drawn, own_key, source, target, blocks, factor):
    owner, partner = [(jnp.arange(drawn.shape[dim]) // (drawn.shape[dim] // blocks)).reshape([-1 if axis == dim else 1 for axis in range(drawn.ndim)]) for dim in (source, target)]
    chosen = jax.random.permutation(own_key, blocks)[partner]
    strong = (owner == chosen) | (owner == (partner + blocks // 2) % blocks)
    return jnp.where(strong, factor * drawn, drawn)


def level_of(stream_key, extent, split, low, top_value):
    def one(dim, blocks):
        draws = jax.random.uniform(jax.random.fold_in(jax.random.fold_in(stream_key, 6), dim), (blocks,), jnp.float32, low / len(split), top_value / len(split))
        return jnp.repeat(jnp.exp(draws), extent[dim] // blocks).reshape((-1,) + (1,) * (len(extent) - dim - 1))

    level = one(*split[0])
    for cut in split[1:]:
        level = level * one(*cut)
    return level


def gaussian(rng, extent, width, reach, split=(), held_as=jnp.bfloat16):
    factor_of = level_of(rng, extent, split, -0.22, 0.18) if split else 1.0
    entries = jax.random.normal(rng, extent, jnp.float32) * width * factor_of
    return jnp.minimum(jnp.maximum(entries, -reach), reach).astype(held_as)


def noise_with(own_key, dims, spread, most, cuts, heavy, held_as=jnp.bfloat16):
    values = spread * jax.random.normal(own_key, dims, jnp.float32)
    if cuts:
        values = values * level_of(own_key, dims, cuts, -0.22, 0.18)
    return jnp.clip(strengthened(values, jax.random.fold_in(own_key, 3), *heavy), -most, most).astype(held_as)


def setup_inputs(seed: int = 0) -> dict:
    splits = jax.random.split(jax.random.key(seed), 8)
    source = gaussian(splits[0], (NZ, NX * NY), 1.0, 6.0, ((0, 8), (1, 4)), jnp.float32)
    z_vectors = noise_with(splits[1], (NZ, NZ), NZ ** -0.5, 0.375, ((0, 8), (1, 4)), (0, 1, 8, 2.0), jnp.float32)
    x_vectors = gaussian(splits[2], (NX, NX), NX ** -0.5, 3.0, (), jnp.float32)
    y_vectors = gaussian(splits[3], (NY, NY), NY ** -0.5, 0.25, (), jnp.float32)
    z_values = jnp.clip(jnp.exp(jax.random.uniform(splits[4], (NZ,), jnp.float32, math.log(0.1), math.log(3.0))), 0.1, 3.0)
    x_values = jnp.clip(jnp.exp(jax.random.uniform(splits[5], (NX,), jnp.float32, math.log(0.1), math.log(3.0))), 0.1, 3.0)
    y_values = jnp.clip(jnp.exp(jax.random.uniform(splits[6], (NY,), jnp.float32, math.log(0.1), math.log(3.0))), 0.1, 3.0)
    return dict(source=source, z_vectors=z_vectors, x_vectors=x_vectors, y_vectors=y_vectors, z_values=z_values, x_values=x_values, y_values=y_values)


def reference(source, z_vectors, x_vectors, y_vectors, z_values, x_values, y_values):
    exact_mode = lax.Precision.HIGHEST
    field = source.reshape(NZ, NX, NY)
    along_y = jnp.einsum("zxy,yj->zxj", field, y_vectors, precision=exact_mode)
    along_x = jnp.einsum("zxj,xi->zij", along_y, x_vectors, precision=exact_mode)
    flat_modes = along_x.reshape(NZ, NX * NY)
    coefficients = lax.dot_general(z_vectors, flat_modes, (((0,), (0,)), ((), ())), precision=exact_mode, preferred_element_type=jnp.float32)
    divisor = z_values[:, None, None] + x_values[None, :, None] + y_values[None, None, :]
    scaled = coefficients.reshape(NZ, NX, NY) / divisor
    back_z = jnp.dot(z_vectors, scaled.reshape(NZ, NX * NY), precision=exact_mode, preferred_element_type=jnp.float32)
    back_x = jnp.einsum("zij,xi->zxj", back_z.reshape(NZ, NX, NY), x_vectors, precision=exact_mode)
    solution = jnp.einsum("zxj,yj->zxy", back_x, y_vectors, precision=exact_mode)
    return solution.reshape(NZ, NX * NY)
```

```python
import functools

import jax
import jax.numpy as jnp
from jax import lax
from jax.experimental import pallas as pl
from jax.experimental.pallas import tpu as pltpu
from jax.sharding import PartitionSpec as P

f32, bf16 = jnp.float32, jnp.bfloat16
MESH = pl.DeviceIdType.MESH


def split(x):
    hi = x.astype(bf16)
    return hi, (x - hi.astype(f32)).astype(bf16)


def dot(a, b, flip):
    dims = (((1,), (1 if flip else 0,)), ((), ()))
    return lax.dot_general(a, b, dims, preferred_element_type=f32)


def product(a, b_hi, b_lo, flip=False):
    rows = a.shape[0]
    a_hi, a_lo = split(a)
    both = dot(jnp.concatenate([a_hi, a_lo], axis=0), b_hi, flip)
    return both[:rows] + (both[rows:] + dot(a_hi, b_lo, flip))


def each(count, body, start=0, down=False):
    if count <= 8:
        order = range(start, count)
        for step in reversed(order) if down else order:
            body(step)
    else:
        lax.fori_loop(
            start, count,
            lambda step, _: (body(count - 1 + start - step if down else step), 0)[1], 0,
        )


def flipped(index, count, d):
    total, unit = 0, 1
    while unit < count:
        total = total + unit * lax.rem(index // unit + d // unit, 2)
        unit *= 2
    return total


def kernel(
    n, m, pack, group,
    source, z_vectors, y_vectors, z_values, y_values, x_vectors, x_values,
    out,
    src, y_raw, y_hi, y_lo, zval, yval, y_col,
    inverse_sum, v, w_hi, w_lo, a_t, fields, partial, inner_in, half, outer_in, final, back,
    load_sem, send_sem, a_sem, v_sem, outer_sem, inner_sem, inner2_sem, r1_sem, r2_sem, q_sem,
):
    g, c = lax.axis_index("gz"), lax.axis_index("col")
    rows, width = src.shape
    lanes = pack * rows
    jr = a_t.shape[1]
    kc = v.shape[2]
    span = width // pack
    inner_bit = lax.rem(c, 2)
    outer_bit = c // 2
    inner = outer_bit * 2 + (1 - inner_bit)
    outer = (1 - outer_bit) * 2 + inner_bit
    across = (1 - outer_bit) * 2 + (1 - inner_bit)

    def at(peer_g, peer_c):
        return {"gz": peer_g, "col": peer_c}

    def send(src_ref, dst_ref, lane, recv, peer):
        pltpu.make_async_remote_copy(
            src_ref=src_ref, dst_ref=dst_ref, send_sem=send_sem.at[lane], recv_sem=recv,
            device_id=peer, device_id_type=MESH,
        ).start()

    def arrived(ref, sem):
        pltpu.make_async_copy(ref, ref, sem).wait()

    barrier = pltpu.get_barrier_semaphore()

    def greet(d):
        pl.semaphore_signal(
            barrier, inc=1, device_id=at(flipped(g, n, d), c), device_id_type=MESH
        )

    each(n, greet, 1, down=True)
    for peer in (outer, inner):
        pl.semaphore_signal(barrier, inc=1, device_id=at(g, peer), device_id_type=MESH)

    pl.semaphore_signal(barrier, inc=1, device_id=at(g, across), device_id_type=MESH)
    loads = [
        pltpu.make_async_copy(a, b, load_sem.at[i])
        for i, (a, b) in enumerate(
            [(z_vectors, v.at[0]), (y_vectors, y_raw), (source, src), (z_values, zval), (y_values, yval)]
        )
    ]
    for copy in loads:
        copy.start()
    loads[1].wait()
    hi, lo = split(y_raw[...])
    y_hi[...] = hi
    y_lo[...] = lo
    loads[2].wait()
    along = product(src[...], hi, lo)
    stacked = jnp.concatenate([along[:, h * span:(h + 1) * span] for h in range(pack)], axis=0)
    a_t[...] = jnp.transpose(stacked).reshape(n, jr, lanes)
    fields[c, 0] = a_t[g]
    loads[0].wait()
    pl.semaphore_wait(barrier, n + 2)

    def send_a(d):
        peer = flipped(g, n, d)
        send(a_t.at[peer], fields.at[c, d], 0, a_sem.at[d], at(peer, c))

    def send_v(held, d):
        send(v.at[held], v.at[held + d], 1, v_sem.at[held + d], at(flipped(g, n, d), c))

    def pass_v(held, unit):
        each(n // 2, lambda e: send_v(0, 2 * e), 1, down=True)
        send_v(0, 1)

    def relay_v(held):
        arrived(v.at[held], v_sem.at[held])
        send_v(held, 1)

    def relay(d, direct=False):
        block = fields.at[c, d]
        send(block, block, 2, outer_sem.at[d], at(g, outer))
        send(block, block, 3, inner_sem.at[d], at(g, inner))
        if direct:
            send(block, block, 4, inner2_sem.at[d], at(g, across))

    def relay_near(d):
        arrived(fields.at[c, d], a_sem.at[d])
        relay(d)

    def relay_far(d):
        arrived(fields.at[c, d], a_sem.at[d])
        relay(d, True)

    def relay_outer(d):
        block = fields.at[outer, d]
        arrived(block, outer_sem.at[d])
        send(block, block, 4, inner2_sem.at[d], at(g, inner))

    def build(d):
        hi, lo = split(v[d])
        for h in range(pack):
            w_hi[d, h * rows:(h + 1) * rows, h * kc:(h + 1) * kc] = hi
            w_lo[d, h * rows:(h + 1) * rows, h * kc:(h + 1) * kc] = lo

    near_count = n // 2
    pass_v(0, n // 2)
    each(n, send_a, 1, down=True)
    relay(0)

    if pack > 1:
        w_hi[...] = jnp.zeros_like(w_hi)
        w_lo[...] = jnp.zeros_like(w_lo)
    build(0)
    loads[3].wait()
    loads[4].wait()
    y_col[...] = jnp.transpose(jnp.broadcast_to(yval[...], (128, width)))
    z_part = zval[:, pl.ds(pl.multiple_of(c * kc, 128), kc)]
    base = jnp.concatenate(
        [
            z_part + y_col[pl.ds(pl.multiple_of(h * span + g * jr, 8), jr), 0:1]
            for h in range(pack)
        ],
        axis=1,
    )
    for i in range(m):
        inverse_sum[i] = 1.0 / (base + x_values[i])

    held, unit = [0], n // 2
    while unit > 1:
        held += [h + unit for h in held]
        unit //= 2
    queue = held[1:]
    if n <= 8:
        for d in range(1, n):
            (relay_near if d < near_count else relay_far)(d)
            if d > 1 and queue:
                relay_v(queue.pop(0))
    for h in queue:
        relay_v(h)
    if n > 8:
        each(near_count, relay_near, 1)
        each(n, relay_far, near_count)
    each(near_count, relay_outer)

    def ready(d):
        arrived(fields.at[inner, d], inner_sem.at[d])
        arrived(fields.at[across, d], inner2_sem.at[d])

    def ready_outer(d):
        arrived(fields.at[outer, d], outer_sem.at[d])

    def received(d):
        if d % 2:
            arrived(v.at[d], v_sem.at[d])
        if d:
            build(d)
        if d >= near_count:
            ready_outer(d)
        ready(d)

    if n > 8:
        each(n // 2, lambda e: build(2 * e), 1)

        def build_odd(e):
            arrived(v.at[2 * e + 1], v_sem.at[2 * e + 1])
            build(2 * e + 1)

        each(n // 2, build_odd)
        each(n, ready_outer, near_count)
        each(n, ready)

    def lhs(first):
        parts = [fields[:, first + s].reshape(m * jr, lanes) for s in range(group)]
        return parts[0] if group == 1 else jnp.concatenate(parts, axis=1)

    def weights(ref, first):
        return ref[pl.ds(first, group)].reshape(group * lanes, pack * kc)

    def term(s):
        if n <= 8:
            for k in range(group):
                received(s * group + k)
        return product(lhs(s * group), weights(w_hi, s * group), weights(w_lo, s * group))

    steps = n // group
    if steps <= 8:
        modes = term(0)
        for s in range(1, steps):
            modes = modes + term(s)
    else:
        modes = lax.fori_loop(1, steps, lambda s, acc: acc + term(s), term(0))

    lines = [modes[x * jr:(x + 1) * jr] for x in range(m)]
    scaled = []
    for i in range(m):
        total = x_vectors[0, i] * lines[0]
        for x in range(1, m):
            total = total + x_vectors[x, i] * lines[x]
        scaled.append(total * inverse_sum[i])
    turned = []
    for x in [o * 2 + b for b in range(2) for o in range(m // 2)]:
        total = x_vectors[x, 0] * scaled[0]
        for i in range(1, m):
            total = total + x_vectors[x, i] * scaled[i]
        turned.append(total)
    turned = jnp.concatenate(turned, axis=0)
    t_hi, t_lo = split(turned)
    t_both = jnp.concatenate([t_hi, t_lo], axis=0)

    def inverse(s):
        first = s * group
        wh, wl = weights(w_hi, first), weights(w_lo, first)
        both = dot(t_both, wh, True)
        values = both[:m * jr] + (both[m * jr:] + dot(t_hi, wl, True))
        for k in reversed(range(group)):
            partial[first + k] = values[:, k * lanes:(k + 1) * lanes].reshape(2, m // 2, jr, lanes)
        for k in reversed(range(group)):
            send(
                partial.at[first + k, 1 - inner_bit], inner_in.at[first + k], 5,
                r1_sem.at[first + k], at(g, inner),
            )

    each(steps, inverse, down=True)

    def fold_inner(d):
        arrived(inner_in.at[d], r1_sem.at[d])
        half[d] = partial[d, inner_bit] + inner_in[d]
        send(half.at[d, 1 - outer_bit], outer_in.at[d], 6, r2_sem.at[d], at(g, outer))

    each(n, fold_inner, down=True)

    def fold_outer(d):
        arrived(outer_in.at[d], r2_sem.at[d])
        final[d] = half[d, outer_bit] + outer_in[d]
        send(final.at[d], back.at[g], 7, q_sem.at[d], at(flipped(g, n, d), c))

    each(n, fold_outer, 1, down=True)
    arrived(outer_in.at[0], r2_sem.at[0])
    back[g] = half[0, outer_bit] + outer_in[0]

    each(n, lambda d: arrived(back.at[flipped(g, n, d)], q_sem.at[d]), 1, down=True)
    turned_back = jnp.transpose(back[...].reshape(n * jr, lanes))
    lines_back = jnp.concatenate(
        [turned_back[h * rows:(h + 1) * rows] for h in range(pack)], axis=1
    ) if pack > 1 else turned_back
    out[...] = product(lines_back, y_hi[...], y_lo[...], True)

    arrived(a_t.at[pl.ds(0, n - 1)], send_sem.at[0])
    arrived(v.at[pl.ds(0, n - 1)], send_sem.at[1])
    for lane in (2, 3, 4):
        arrived(fields.at[c], send_sem.at[lane])
    arrived(inner_in, send_sem.at[5])
    arrived(outer_in, send_sem.at[6])
    arrived(final.at[pl.ds(0, n - 1)], send_sem.at[7])


def shards(n, m, source, z_vectors, x_vectors, y_vectors, z_values, x_values, y_values):
    rows, width = source.shape
    kc = z_vectors.shape[1]
    pack = max(1, 128 // rows)
    while pack > 1 and width % (n * pack * 8):
        pack //= 2
    lanes, jr = pack * rows, width // (n * pack)
    group = 2 if lanes % 128 == 0 and n % 2 == 0 else 1
    vm = pltpu.VMEM
    dma = pltpu.SemaphoreType.DMA
    hbm, smem = pl.BlockSpec(memory_space=pl.ANY), pl.BlockSpec(memory_space=pltpu.SMEM)
    return pl.pallas_call(
        functools.partial(kernel, n, m, pack, group),
        out_shape=jax.ShapeDtypeStruct((rows, width), f32),
        in_specs=[hbm] * 5 + [smem] * 2,
        out_specs=pl.BlockSpec(memory_space=vm),
        scratch_shapes=[
            vm((rows, width), f32),
            vm(y_vectors.shape, f32),
            vm(y_vectors.shape, bf16),
            vm(y_vectors.shape, bf16),
            vm((1, z_values.shape[0]), f32),
            vm((1, width), f32),
            vm((width, 128), f32),
            vm((m, jr, pack * kc), f32),
            vm((n, rows, kc), f32),
            vm((n, lanes, pack * kc), bf16),
            vm((n, lanes, pack * kc), bf16),
            vm((n, jr, lanes), f32),
            vm((m, n, jr, lanes), f32),
            vm((n, 2, m // 2, jr, lanes), f32),
            vm((n, m // 2, jr, lanes), f32),
            vm((n, m // 2, jr, lanes), f32),
            vm((n, jr, lanes), f32),
            vm((n, jr, lanes), f32),
            vm((n, jr, lanes), f32),
            dma((5,)),
            dma((8,)),
        ] + [dma((n,))] * 8,
        compiler_params=pltpu.CompilerParams(
            collective_id=0, has_side_effects=True, vmem_limit_bytes=60 * 1024 * 1024
        ),
    )(
        source, z_vectors, y_vectors, z_values.reshape(1, -1), y_values.reshape(1, -1),
        x_vectors, x_values,
    )


def bits(index, count):
    deltas, unit = [], 1
    while unit < count:
        deltas.append(unit * (1 - 2 * lax.rem(index // unit, 2)))
        unit *= 2
    return deltas


def moved(index, deltas, d):
    for place, delta in enumerate(deltas):
        if d >> place & 1:
            index = index + delta
    return index


def whole_kernel(
    n, m,
    source, z_vectors, y_vectors, z_values, y_values, x_vectors, x_values,
    out,
    src, y_raw, y_hi, y_lo, zval, yval, y_col,
    inverse_sum, v, w_hi, w_lo, a_t, fields, partial, back,
    load_sem, send_sem, a_sem, q_sem, line_sem, x_sem, y_sem, corner_sem, core_sem,
):
    g, c = lax.axis_index("gz"), lax.axis_index("col")
    rows, width = src.shape
    kc = v.shape[2]
    jr, lanes = a_t.shape[1:]
    span = width // 2
    order = n * rows
    half = rows // 2
    g_bits, c_bits = bits(g, n), bits(c, m)
    me = g * m + c

    def at(d):
        return {"gz": moved(g, g_bits, d // m), "col": moved(c, c_bits, d % m)}

    def slot(d):
        return moved(g, g_bits, d // m) * m + moved(c, c_bits, d % m)

    def send(src_ref, dst_ref, lane, recv, peer):
        pltpu.make_async_remote_copy(
            src_ref=src_ref, dst_ref=dst_ref, send_sem=send_sem.at[lane], recv_sem=recv,
            device_id=peer, device_id_type=MESH,
        ).start()

    def arrived(ref, sem):
        pltpu.make_async_copy(ref, ref, sem).wait()

    loads = [
        pltpu.make_async_copy(a, b, load_sem.at[i])
        for i, (a, b) in enumerate(
            [(z_vectors, v.at[me]), (y_vectors, y_raw), (source, src), (z_values, zval), (y_values, yval)]
        )
    ]
    for copy in loads:
        copy.start()
    barrier = pltpu.get_barrier_semaphore()
    far = sorted(range(1, n * m), key=lambda d: -bin(d).count("1") - (d // m // 2))
    for d in far:
        pl.semaphore_signal(barrier, inc=1, device_id=at(d), device_id_type=MESH)

    loads[1].wait()
    hi, lo = split(y_raw[...])
    y_hi[...] = hi
    y_lo[...] = lo
    loads[2].wait()
    along = product(src[...], hi, lo)
    stacked = jnp.concatenate([along[:, :span], along[:, span:]], axis=0)
    a_t[...] = jnp.transpose(stacked).reshape(n * m, jr, lanes)
    fields[me] = a_t[me]
    loads[0].wait()
    pl.semaphore_wait(barrier, n * m - 1)

    to_x, to_y, to_core = m, 2, 1
    line = [e * m for e in range(0, n, 2)]

    def relay(block, lane, sem, d):
        send(v.at[block], v.at[block], lane, sem, at(d))

    for i in reversed(range(1, len(line))):
        relay(me, 0, line_sem.at[i], line[i])
    relay(me, 0, x_sem.at[0], to_x)
    relay(me, 0, y_sem.at[0], to_y)
    for d in far:
        send(a_t.at[slot(d)], fields.at[me], 1, a_sem, at(d))
    relay(me, 0, core_sem.at[0, 0], to_core)

    def build(block_g, block_c):
        hi, lo = split(v[block_g * m + block_c])
        across = pl.ds(pl.multiple_of(block_c * kc, 128), kc)
        down = pl.ds(pl.multiple_of(block_g * rows, 16), rows)
        w_hi[down, across] = hi
        w_lo[down, across] = lo

    def build_at(d):
        build(moved(g, g_bits, d // m), moved(c, c_bits, d % m))

    def take_line(i):
        block = slot(line[i])
        if i:
            arrived(v.at[block], line_sem.at[i])
            relay(block, 0, x_sem.at[i], to_x)
            relay(block, 0, y_sem.at[i], to_y)
            relay(block, 0, core_sem.at[0, i], to_core)
        build_at(line[i])

    def take_x(i):
        block = slot(line[i] + to_x)
        arrived(v.at[block], x_sem.at[i])
        part = v.at[block, pl.ds(0, half)]
        send(part, part, 0, corner_sem.at[0, i], at(to_y))
        relay(block, 0, core_sem.at[1, i], to_core)
        build_at(line[i] + to_x)

    def take_y(i):
        block = slot(line[i] + to_y)
        arrived(v.at[block], y_sem.at[i])
        part = v.at[block, pl.ds(half, half)]
        send(part, part, 0, corner_sem.at[1, i], at(to_x))
        relay(block, 0, core_sem.at[2, i], to_core)
        build_at(line[i] + to_y)

    def take_corner(i):
        block = slot(line[i] + to_x + to_y)
        for k in range(2):
            part = v.at[block, pl.ds(k * half, half)]
            arrived(part, corner_sem.at[k, i])
        relay(block, 0, core_sem.at[3, i], to_core)
        build_at(line[i] + to_x + to_y)

    for i in range(len(line)):
        take_line(i)
        take_x(i)
        take_y(i)
        if i:
            take_corner(i - 1)

    loads[3].wait()
    loads[4].wait()
    y_col[...] = jnp.transpose(jnp.broadcast_to(yval[...], (128, width)))
    base = jnp.concatenate(
        [y_col[pl.ds(pl.multiple_of(h * span + me * jr, 8), jr), 0:1] for h in range(2)], axis=0
    ) + zval[...]
    for i in range(m):
        inverse_sum[i] = 1.0 / (base + x_values[i])
    take_corner(len(line) - 1)

    for i in range(len(line)):
        for k, d in enumerate([0, to_x, to_y, to_x + to_y]):
            arrived(v.at[slot(line[i] + d + to_core)], core_sem.at[k, i])
            build_at(line[i] + d + to_core)

    low = lax.broadcasted_iota(jnp.int32, (jr, lanes), 1) < rows
    arrived(fields.at[pl.ds(0, n * m - 1)], a_sem)

    def pair(a, b):
        return (
            jnp.where(low, a, pltpu.roll(b, rows, axis=1)),
            jnp.where(low, pltpu.roll(a, rows, axis=1), b),
        )

    stack = []
    for x in range(m):
        pairs = [pair(fields[2 * t * m + x], fields[(2 * t + 1) * m + x]) for t in range(n // 2)]
        for h in range(2):
            stack.append(jnp.concatenate([both[h] for both in pairs], axis=1))
    modes = product(jnp.concatenate(stack, axis=0), w_hi[...], w_lo[...])

    deep = 2 * jr
    lines = [modes[x * deep:(x + 1) * deep] for x in range(m)]
    scaled = []
    for i in range(m):
        total = x_vectors[0, i] * lines[0]
        for x in range(1, m):
            total = total + x_vectors[x, i] * lines[x]
        scaled.append(total * inverse_sum[i])
    turned = []
    for x in range(m):
        total = x_vectors[x, 0] * scaled[0]
        for i in range(1, m):
            total = total + x_vectors[x, i] * scaled[i]
        turned.append(total)
    turned = jnp.concatenate(turned, axis=0)
    t_hi, t_lo = split(turned)
    t_both = jnp.concatenate([t_hi, t_lo], axis=0)

    both = dot(t_both, w_hi[...], True)
    values = both[:m * deep] + (both[m * deep:] + dot(t_hi, w_lo[...], True))
    for t in range(n // 2):
        for x in range(m):
            ends = [values[x * deep + h * jr:x * deep + (h + 1) * jr, t * lanes:(t + 1) * lanes] for h in range(2)]
            even, odd = pair(*ends)
            partial[2 * t * m + x] = even
            partial[(2 * t + 1) * m + x] = odd
    for d in far:
        send(partial.at[slot(d)], back.at[me], 2, q_sem, at(d))
    back[me] = partial[me]

    arrived(back.at[pl.ds(0, n * m - 1)], q_sem)
    turned_back = jnp.transpose(back[...].reshape(n * m * jr, lanes))
    lines_back = jnp.concatenate([turned_back[:rows], turned_back[rows:]], axis=1)
    out[...] = product(lines_back, y_hi[...], y_lo[...], True)

    arrived(v.at[pl.ds(0, n * m - 1)], send_sem.at[0])
    arrived(fields.at[pl.ds(0, n * m - 1)], send_sem.at[1])
    arrived(back.at[pl.ds(0, n * m - 1)], send_sem.at[2])


def whole_shards(n, m, source, z_vectors, x_vectors, y_vectors, z_values, x_values, y_values):
    rows, width = source.shape
    kc = z_vectors.shape[1]
    jr, lanes, order = width // (2 * n * m), 2 * rows, n * rows
    vm = pltpu.VMEM
    dma = pltpu.SemaphoreType.DMA
    hbm, smem = pl.BlockSpec(memory_space=pl.ANY), pl.BlockSpec(memory_space=pltpu.SMEM)
    tiles = (n * m, jr, lanes)
    return pl.pallas_call(
        functools.partial(whole_kernel, n, m),
        out_shape=jax.ShapeDtypeStruct((rows, width), f32),
        in_specs=[hbm] * 5 + [smem] * 2,
        out_specs=pl.BlockSpec(memory_space=vm),
        scratch_shapes=[
            vm((rows, width), f32),
            vm(y_vectors.shape, f32),
            vm(y_vectors.shape, bf16),
            vm(y_vectors.shape, bf16),
            vm((1, order), f32),
            vm((1, width), f32),
            vm((width, 128), f32),
            vm((m, 2 * jr, order), f32),
            vm((n * m, rows, kc), f32),
            vm((order, order), bf16),
            vm((order, order), bf16),
            vm(tiles, f32),
            vm(tiles, f32),
            vm(tiles, f32),
            vm(tiles, f32),
            dma((5,)),
            dma((3,)),
            dma,
            dma,
            dma((n // 2,)),
            dma((n // 2,)),
            dma((n // 2,)),
            dma((2, n // 2)),
            dma((4, n // 2)),
        ],
        compiler_params=pltpu.CompilerParams(
            collective_id=0, has_side_effects=True, vmem_limit_bytes=60 * 1024 * 1024
        ),
    )(
        source, z_vectors, y_vectors, z_values.reshape(1, -1), y_values.reshape(1, -1),
        x_vectors, x_values,
    )


def fits_whole(n, m, source, z_vectors):
    rows, width = source.shape
    order = z_vectors.shape[0] * n
    return (
        rows == 64 and m == 4 and n <= 8 and n % 2 == 0 and order * order <= 1 << 20
        and z_vectors.shape[1] % 128 == 0 and width % (16 * n * m) == 0
    )


def solution(mesh):
    placed = (P("gz", "col"), P("gz", "col"), P(), P(), P(), P(), P())
    sizes = (mesh.shape["gz"], mesh.shape["col"])

    def body(source, z_vectors, *rest):
        chosen = whole_shards if fits_whole(*sizes, source, z_vectors) else shards
        return chosen(*sizes, source, z_vectors, *rest)

    return jax.shard_map(
        body,
        mesh=mesh, in_specs=placed, out_specs=P("gz", "col"), check_vma=False,
    )
```

```python
import functools

import jax
import jax.numpy as jnp
from jax import lax
from jax.experimental import pallas as pl
from jax.experimental.pallas import tpu as pltpu
from jax.sharding import PartitionSpec as P

f32, bf16 = jnp.float32, jnp.bfloat16
MESH = pl.DeviceIdType.MESH


def split(x):
    hi = x.astype(bf16)
    return hi, (x - hi.astype(f32)).astype(bf16)


def dot(a, b, flip):
    dims = (((1,), (1 if flip else 0,)), ((), ()))
    return lax.dot_general(a, b, dims, preferred_element_type=f32)


def product(a, b_hi, b_lo, flip=False):
    rows = a.shape[0]
    a_hi, a_lo = split(a)
    both = dot(jnp.concatenate([a_hi, a_lo], axis=0), b_hi, flip)
    return both[:rows] + (both[rows:] + dot(a_hi, b_lo, flip))


def each(count, body, start=0, down=False):
    if count <= 8:
        order = range(start, count)
        for step in reversed(order) if down else order:
            body(step)
    else:
        lax.fori_loop(
            start, count,
            lambda step, _: (body(count - 1 + start - step if down else step), 0)[1], 0,
        )


def flipped(index, count, d):
    total, unit = 0, 1
    while unit < count:
        total = total + unit * lax.rem(index // unit + d // unit, 2)
        unit *= 2
    return total


def kernel(
    n, m, pack, group,
    source, z_vectors, y_vectors, z_values, y_values, x_vectors, x_values,
    out,
    src, y_raw, y_hi, y_lo, zval, yval, y_col,
    inverse_sum, v, w_hi, w_lo, a_t, fields, partial, inner_in, half, outer_in, final, back,
    load_sem, send_sem, a_sem, v_sem, outer_sem, inner_sem, inner2_sem, r1_sem, r2_sem, q_sem,
):
    g, c = lax.axis_index("gz"), lax.axis_index("col")
    rows, width = src.shape
    lanes = pack * rows
    jr = a_t.shape[1]
    kc = v.shape[2]
    span = width // pack
    inner_bit = lax.rem(c, 2)
    outer_bit = c // 2
    inner = outer_bit * 2 + (1 - inner_bit)
    outer = (1 - outer_bit) * 2 + inner_bit
    across = (1 - outer_bit) * 2 + (1 - inner_bit)

    def at(peer_g, peer_c):
        return {"gz": peer_g, "col": peer_c}

    def send(src_ref, dst_ref, lane, recv, peer):
        pltpu.make_async_remote_copy(
            src_ref=src_ref, dst_ref=dst_ref, send_sem=send_sem.at[lane], recv_sem=recv,
            device_id=peer, device_id_type=MESH,
        ).start()

    def arrived(ref, sem):
        pltpu.make_async_copy(ref, ref, sem).wait()

    barrier = pltpu.get_barrier_semaphore()

    def greet(d):
        pl.semaphore_signal(
            barrier, inc=1, device_id=at(flipped(g, n, d), c), device_id_type=MESH
        )

    each(n, greet, 1, down=True)
    for peer in (outer, inner):
        pl.semaphore_signal(barrier, inc=1, device_id=at(g, peer), device_id_type=MESH)

    pl.semaphore_signal(barrier, inc=1, device_id=at(g, across), device_id_type=MESH)
    loads = [
        pltpu.make_async_copy(a, b, load_sem.at[i])
        for i, (a, b) in enumerate(
            [(z_vectors, v.at[0]), (y_vectors, y_raw), (source, src), (z_values, zval), (y_values, yval)]
        )
    ]
    for copy in loads:
        copy.start()
    loads[1].wait()
    hi, lo = split(y_raw[...])
    y_hi[...] = hi
    y_lo[...] = lo
    loads[2].wait()
    along = product(src[...], hi, lo)
    stacked = jnp.concatenate([along[:, h * span:(h + 1) * span] for h in range(pack)], axis=0)
    a_t[...] = jnp.transpose(stacked).reshape(n, jr, lanes)
    fields[c, 0] = a_t[g]
    loads[0].wait()
    pl.semaphore_wait(barrier, n + 2)

    def send_a(d):
        peer = flipped(g, n, d)
        send(a_t.at[peer], fields.at[c, d], 0, a_sem.at[d], at(peer, c))

    def send_v(held, d):
        send(v.at[held], v.at[held + d], 1, v_sem.at[held + d], at(flipped(g, n, d), c))

    def pass_v(held, unit):
        each(n // 2, lambda e: send_v(0, 2 * e), 1, down=True)
        send_v(0, 1)

    def relay_v(held):
        arrived(v.at[held], v_sem.at[held])
        send_v(held, 1)

    def relay(d, direct=False):
        block = fields.at[c, d]
        send(block, block, 2, outer_sem.at[d], at(g, outer))
        send(block, block, 3, inner_sem.at[d], at(g, inner))
        if direct:
            send(block, block, 4, inner2_sem.at[d], at(g, across))

    def relay_near(d):
        arrived(fields.at[c, d], a_sem.at[d])
        relay(d)

    def relay_far(d):
        arrived(fields.at[c, d], a_sem.at[d])
        relay(d, True)

    def relay_outer(d):
        block = fields.at[outer, d]
        arrived(block, outer_sem.at[d])
        send(block, block, 4, inner2_sem.at[d], at(g, inner))

    def build(d):
        hi, lo = split(v[d])
        for h in range(pack):
            w_hi[d, h * rows:(h + 1) * rows, h * kc:(h + 1) * kc] = hi
            w_lo[d, h * rows:(h + 1) * rows, h * kc:(h + 1) * kc] = lo

    near_count = n // 2
    pass_v(0, n // 2)
    each(n, send_a, 1, down=True)
    relay(0)

    if pack > 1:
        w_hi[...] = jnp.zeros_like(w_hi)
        w_lo[...] = jnp.zeros_like(w_lo)
    build(0)
    loads[3].wait()
    loads[4].wait()
    y_col[...] = jnp.transpose(jnp.broadcast_to(yval[...], (128, width)))
    z_part = zval[:, pl.ds(pl.multiple_of(c * kc, 128), kc)]
    base = jnp.concatenate(
        [
            z_part + y_col[pl.ds(pl.multiple_of(h * span + g * jr, 8), jr), 0:1]
            for h in range(pack)
        ],
        axis=1,
    )
    for i in range(m):
        inverse_sum[i] = 1.0 / (base + x_values[i])

    held, unit = [0], n // 2
    while unit > 1:
        held += [h + unit for h in held]
        unit //= 2
    queue = held[1:]
    if n <= 8:
        for d in range(1, n):
            (relay_near if d < near_count else relay_far)(d)
            if d > 1 and queue:
                relay_v(queue.pop(0))
    for h in queue:
        relay_v(h)
    if n > 8:
        each(near_count, relay_near, 1)
        each(n, relay_far, near_count)
    each(near_count, relay_outer)

    def ready(d):
        arrived(fields.at[inner, d], inner_sem.at[d])
        arrived(fields.at[across, d], inner2_sem.at[d])

    def ready_outer(d):
        arrived(fields.at[outer, d], outer_sem.at[d])

    def received(d):
        if d % 2:
            arrived(v.at[d], v_sem.at[d])
        if d:
            build(d)
        if d >= near_count:
            ready_outer(d)
        ready(d)

    if n > 8:
        each(n // 2, lambda e: build(2 * e), 1)

        def build_odd(e):
            arrived(v.at[2 * e + 1], v_sem.at[2 * e + 1])
            build(2 * e + 1)

        each(n // 2, build_odd)
        each(n, ready_outer, near_count)
        each(n, ready)

    def lhs(first):
        parts = [fields[:, first + s].reshape(m * jr, lanes) for s in range(group)]
        return parts[0] if group == 1 else jnp.concatenate(parts, axis=1)

    def weights(ref, first):
        return ref[pl.ds(first, group)].reshape(group * lanes, pack * kc)

    def term(s):
        if n <= 8:
            for k in range(group):
                received(s * group + k)
        return product(lhs(s * group), weights(w_hi, s * group), weights(w_lo, s * group))

    steps = n // group
    if steps <= 8:
        modes = term(0)
        for s in range(1, steps):
            modes = modes + term(s)
    else:
        modes = lax.fori_loop(1, steps, lambda s, acc: acc + term(s), term(0))

    lines = [modes[x * jr:(x + 1) * jr] for x in range(m)]
    scaled = []
    for i in range(m):
        total = x_vectors[0, i] * lines[0]
        for x in range(1, m):
            total = total + x_vectors[x, i] * lines[x]
        scaled.append(total * inverse_sum[i])
    turned = []
    for x in [o * 2 + b for b in range(2) for o in range(m // 2)]:
        total = x_vectors[x, 0] * scaled[0]
        for i in range(1, m):
            total = total + x_vectors[x, i] * scaled[i]
        turned.append(total)
    turned = jnp.concatenate(turned, axis=0)
    t_hi, t_lo = split(turned)
    t_both = jnp.concatenate([t_hi, t_lo], axis=0)

    def inverse(s):
        first = s * group
        wh, wl = weights(w_hi, first), weights(w_lo, first)
        both = dot(t_both, wh, True)
        values = both[:m * jr] + (both[m * jr:] + dot(t_hi, wl, True))
        for k in reversed(range(group)):
            partial[first + k] = values[:, k * lanes:(k + 1) * lanes].reshape(2, m // 2, jr, lanes)
        for k in reversed(range(group)):
            send(
                partial.at[first + k, 1 - inner_bit], inner_in.at[first + k], 5,
                r1_sem.at[first + k], at(g, inner),
            )

    each(steps, inverse, down=True)

    def fold_inner(d):
        arrived(inner_in.at[d], r1_sem.at[d])
        half[d] = partial[d, inner_bit] + inner_in[d]
        send(half.at[d, 1 - outer_bit], outer_in.at[d], 6, r2_sem.at[d], at(g, outer))

    each(n, fold_inner, down=True)

    def fold_outer(d):
        arrived(outer_in.at[d], r2_sem.at[d])
        final[d] = half[d, outer_bit] + outer_in[d]
        send(final.at[d], back.at[g], 7, q_sem.at[d], at(flipped(g, n, d), c))

    each(n, fold_outer, 1, down=True)
    arrived(outer_in.at[0], r2_sem.at[0])
    back[g] = half[0, outer_bit] + outer_in[0]

    each(n, lambda d: arrived(back.at[flipped(g, n, d)], q_sem.at[d]), 1, down=True)
    turned_back = jnp.transpose(back[...].reshape(n * jr, lanes))
    lines_back = jnp.concatenate(
        [turned_back[h * rows:(h + 1) * rows] for h in range(pack)], axis=1
    ) if pack > 1 else turned_back
    out[...] = product(lines_back, y_hi[...], y_lo[...], True)

    arrived(a_t.at[pl.ds(0, n - 1)], send_sem.at[0])
    arrived(v.at[pl.ds(0, n - 1)], send_sem.at[1])
    for lane in (2, 3, 4):
        arrived(fields.at[c], send_sem.at[lane])
    arrived(inner_in, send_sem.at[5])
    arrived(outer_in, send_sem.at[6])
    arrived(final.at[pl.ds(0, n - 1)], send_sem.at[7])


def shards(n, m, source, z_vectors, x_vectors, y_vectors, z_values, x_values, y_values):
    rows, width = source.shape
    kc = z_vectors.shape[1]
    pack = max(1, 128 // rows)
    while pack > 1 and width % (n * pack * 8):
        pack //= 2
    lanes, jr = pack * rows, width // (n * pack)
    group = 2 if lanes % 128 == 0 and n % 2 == 0 else 1
    vm = pltpu.VMEM
    dma = pltpu.SemaphoreType.DMA
    hbm, smem = pl.BlockSpec(memory_space=pl.ANY), pl.BlockSpec(memory_space=pltpu.SMEM)
    return pl.pallas_call(
        functools.partial(kernel, n, m, pack, group),
        out_shape=jax.ShapeDtypeStruct((rows, width), f32),
        in_specs=[hbm] * 5 + [smem] * 2,
        out_specs=pl.BlockSpec(memory_space=vm),
        scratch_shapes=[
            vm((rows, width), f32),
            vm(y_vectors.shape, f32),
            vm(y_vectors.shape, bf16),
            vm(y_vectors.shape, bf16),
            vm((1, z_values.shape[0]), f32),
            vm((1, width), f32),
            vm((width, 128), f32),
            vm((m, jr, pack * kc), f32),
            vm((n, rows, kc), f32),
            vm((n, lanes, pack * kc), bf16),
            vm((n, lanes, pack * kc), bf16),
            vm((n, jr, lanes), f32),
            vm((m, n, jr, lanes), f32),
            vm((n, 2, m // 2, jr, lanes), f32),
            vm((n, m // 2, jr, lanes), f32),
            vm((n, m // 2, jr, lanes), f32),
            vm((n, jr, lanes), f32),
            vm((n, jr, lanes), f32),
            vm((n, jr, lanes), f32),
            dma((5,)),
            dma((8,)),
        ] + [dma((n,))] * 8,
        compiler_params=pltpu.CompilerParams(
            collective_id=0, has_side_effects=True, vmem_limit_bytes=60 * 1024 * 1024
        ),
    )(
        source, z_vectors, y_vectors, z_values.reshape(1, -1), y_values.reshape(1, -1),
        x_vectors, x_values,
    )


def bits(index, count):
    deltas, unit = [], 1
    while unit < count:
        deltas.append(unit * (1 - 2 * lax.rem(index // unit, 2)))
        unit *= 2
    return deltas


def moved(index, deltas, d):
    for place, delta in enumerate(deltas):
        if d >> place & 1:
            index = index + delta
    return index


def whole_kernel(
    n, m,
    source, z_vectors, y_vectors, z_values, y_values, x_vectors_in, x_values_in,
    out,
    src, y_raw, y_hi, y_lo, zval, yval, x_vectors, x_values, y_col,
    inverse_sum, v, w_hi, w_lo, a_t, fields, partial, back,
    load_sem, send_sem, a_sem, q_sem, line_sem, x_sem, y_sem, corner_sem, core_sem,
    known_sem,
):
    g, c = lax.axis_index("gz"), lax.axis_index("col")
    rows, width = src.shape
    kc = v.shape[2]
    jr, lanes = a_t.shape[1:]
    span = width // 2
    order = n * rows
    half = rows // 2
    g_bits, c_bits = bits(g, n), bits(c, m)
    me = g * m + c

    def at(d):
        return {"gz": moved(g, g_bits, d // m), "col": moved(c, c_bits, d % m)}

    def slot(d):
        return moved(g, g_bits, d // m) * m + moved(c, c_bits, d % m)

    def send(src_ref, dst_ref, lane, recv, peer):
        pltpu.make_async_remote_copy(
            src_ref=src_ref, dst_ref=dst_ref, send_sem=send_sem.at[lane], recv_sem=recv,
            device_id=peer, device_id_type=MESH,
        ).start()

    def arrived(ref, sem):
        pltpu.make_async_copy(ref, ref, sem).wait()

    loads = [
        pltpu.make_async_copy(a, b, load_sem.at[i])
        for i, (a, b) in enumerate(
            [(z_vectors, v.at[me]), (y_vectors, y_raw), (source, src), (z_values, zval), (y_values, yval),
             (x_vectors_in, x_vectors), (x_values_in, x_values)]
        )
    ]
    to_x, to_y, to_core = m, 2, 1
    line = [e * m for e in range(0, n, 2)]
    barrier = pltpu.get_barrier_semaphore()
    for d in line[:0:-1] + [to_x, to_y, to_core]:
        pl.semaphore_signal(barrier, inc=1, device_id=at(d), device_id_type=MESH)
    for copy in loads:
        copy.start()
    far = sorted(range(1, n * m), key=lambda d: -bin(d).count("1") - (d // m // 2))
    def relay(block, lane, sem, d):
        send(v.at[block], v.at[block], lane, sem, at(d))

    def tell(k):
        pl.semaphore_signal(
            known_sem.at[k], inc=1, device_id=at([to_x, to_y, to_core][k]), device_id_type=MESH
        )

    pl.semaphore_wait(barrier, len(line) + 2)
    tell(0)
    loads[0].wait()
    for i in reversed(range(1, len(line))):
        relay(me, 0, line_sem.at[i], line[i])
    relay(me, 0, x_sem.at[0], to_x)
    relay(me, 0, y_sem.at[0], to_y)
    relay(me, 0, core_sem.at[0, 0], to_core)
    loads[1].wait()
    hi, lo = split(y_raw[...])
    y_hi[...] = hi
    y_lo[...] = lo
    loads[2].wait()
    along = product(src[...], hi, lo)
    stacked = jnp.concatenate([along[:, :span], along[:, span:]], axis=0)
    a_t[...] = jnp.transpose(stacked).reshape(n * m, jr, lanes)
    fields[me] = a_t[me]
    for k, d in enumerate([to_x, to_y, to_core]):
        pl.semaphore_wait(known_sem.at[k], 1)
        if d != to_core:
            tell(k + 1)
    for d in far:
        send(a_t.at[slot(d)], fields.at[me], 1, a_sem, at(d))

    def build(block_g, block_c):
        hi, lo = split(v[block_g * m + block_c])
        across = pl.ds(pl.multiple_of(block_c * kc, 128), kc)
        down = pl.ds(pl.multiple_of(block_g * rows, 16), rows)
        w_hi[down, across] = hi
        w_lo[down, across] = lo

    def build_at(d):
        build(moved(g, g_bits, d // m), moved(c, c_bits, d % m))

    def forward_line(i):
        block = slot(line[i])
        arrived(v.at[block], line_sem.at[i])
        relay(block, 0, x_sem.at[i], to_x)
        relay(block, 0, y_sem.at[i], to_y)
        relay(block, 0, core_sem.at[0, i], to_core)

    def forward_x(i):
        block = slot(line[i] + to_x)
        arrived(v.at[block], x_sem.at[i])
        part = v.at[block, pl.ds(0, half)]
        send(part, part, 0, corner_sem.at[0, i], at(to_y))
        relay(block, 0, core_sem.at[1, i], to_core)

    def forward_y(i):
        block = slot(line[i] + to_y)
        arrived(v.at[block], y_sem.at[i])
        part = v.at[block, pl.ds(half, half)]
        send(part, part, 0, corner_sem.at[1, i], at(to_x))
        relay(block, 0, core_sem.at[2, i], to_core)

    def take_corner(i):
        block = slot(line[i] + to_x + to_y)
        for k in range(2):
            part = v.at[block, pl.ds(k * half, half)]
            arrived(part, corner_sem.at[k, i])
        relay(block, 0, core_sem.at[3, i], to_core)
        build_at(line[i] + to_x + to_y)

    for i in range(1, len(line)):
        forward_line(i)
    for i in range(len(line)):
        forward_x(i)
        forward_y(i)
    for i in range(len(line)):
        for d in (0, to_x, to_y):
            build_at(line[i] + d)

    loads[3].wait()
    for copy in loads[4:]:
        copy.wait()
    y_col[...] = jnp.transpose(jnp.broadcast_to(yval[...], (128, width)))
    base = jnp.concatenate(
        [y_col[pl.ds(pl.multiple_of(h * span + me * jr, 8), jr), 0:1] for h in range(2)], axis=0
    ) + zval[...]
    for i in range(m):
        inverse_sum[i] = 1.0 / (base + x_values[i])
    for i in range(len(line)):
        take_corner(i)

    for i in range(len(line)):
        for k, d in enumerate([0, to_x, to_y, to_x + to_y]):
            arrived(v.at[slot(line[i] + d + to_core)], core_sem.at[k, i])
            build_at(line[i] + d + to_core)

    low = lax.broadcasted_iota(jnp.int32, (jr, lanes), 1) < rows
    arrived(fields.at[pl.ds(0, n * m - 1)], a_sem)

    def pair(a, b):
        return (
            jnp.where(low, a, pltpu.roll(b, rows, axis=1)),
            jnp.where(low, pltpu.roll(a, rows, axis=1), b),
        )

    stack = []
    for x in range(m):
        pairs = [pair(fields[2 * t * m + x], fields[(2 * t + 1) * m + x]) for t in range(n // 2)]
        for h in range(2):
            stack.append(jnp.concatenate([both[h] for both in pairs], axis=1))
    modes = product(jnp.concatenate(stack, axis=0), w_hi[...], w_lo[...])

    deep = 2 * jr
    lines = [modes[x * deep:(x + 1) * deep] for x in range(m)]
    scaled = []
    for i in range(m):
        total = x_vectors[0, i] * lines[0]
        for x in range(1, m):
            total = total + x_vectors[x, i] * lines[x]
        scaled.append(total * inverse_sum[i])
    turned = []
    for x in range(m):
        total = x_vectors[x, 0] * scaled[0]
        for i in range(1, m):
            total = total + x_vectors[x, i] * scaled[i]
        turned.append(total)
    turned = jnp.concatenate(turned, axis=0)
    t_hi, t_lo = split(turned)
    t_both = jnp.concatenate([t_hi, t_lo], axis=0)

    both = dot(t_both, w_hi[...], True)
    values = both[:m * deep] + (both[m * deep:] + dot(t_hi, w_lo[...], True))
    for t in range(n // 2):
        for x in range(m):
            ends = [values[x * deep + h * jr:x * deep + (h + 1) * jr, t * lanes:(t + 1) * lanes] for h in range(2)]
            even, odd = pair(*ends)
            partial[2 * t * m + x] = even
            partial[(2 * t + 1) * m + x] = odd
    for d in far:
        send(partial.at[slot(d)], back.at[me], 2, q_sem, at(d))
    back[me] = partial[me]

    arrived(back.at[pl.ds(0, n * m - 1)], q_sem)
    turned_back = jnp.transpose(back[...].reshape(n * m * jr, lanes))
    lines_back = jnp.concatenate([turned_back[:rows], turned_back[rows:]], axis=1)
    out[...] = product(lines_back, y_hi[...], y_lo[...], True)

    arrived(v.at[pl.ds(0, n * m - 1)], send_sem.at[0])
    arrived(fields.at[pl.ds(0, n * m - 1)], send_sem.at[1])
    arrived(back.at[pl.ds(0, n * m - 1)], send_sem.at[2])


def whole_shards(n, m, source, z_vectors, x_vectors, y_vectors, z_values, x_values, y_values):
    rows, width = source.shape
    kc = z_vectors.shape[1]
    jr, lanes, order = width // (2 * n * m), 2 * rows, n * rows
    vm = pltpu.VMEM
    dma = pltpu.SemaphoreType.DMA
    hbm = pl.BlockSpec(memory_space=pl.ANY)
    tiles = (n * m, jr, lanes)
    return pl.pallas_call(
        functools.partial(whole_kernel, n, m),
        out_shape=jax.ShapeDtypeStruct((rows, width), f32),
        in_specs=[hbm] * 7,
        out_specs=pl.BlockSpec(memory_space=vm),
        scratch_shapes=[
            vm((rows, width), f32),
            vm(y_vectors.shape, f32),
            vm(y_vectors.shape, bf16),
            vm(y_vectors.shape, bf16),
            vm((1, order), f32),
            vm((1, width), f32),
            pltpu.SMEM(x_vectors.shape, f32),
            pltpu.SMEM(x_values.shape, f32),
            vm((width, 128), f32),
            vm((m, 2 * jr, order), f32),
            vm((n * m, rows, kc), f32),
            vm((order, order), bf16),
            vm((order, order), bf16),
            vm(tiles, f32),
            vm(tiles, f32),
            vm(tiles, f32),
            vm(tiles, f32),
            dma((7,)),
            dma((3,)),
            dma,
            dma,
            dma((n // 2,)),
            dma((n // 2,)),
            dma((n // 2,)),
            dma((2, n // 2)),
            dma((4, n // 2)),
            pltpu.SemaphoreType.REGULAR((3,)),
        ],
        compiler_params=pltpu.CompilerParams(
            collective_id=0, has_side_effects=True, vmem_limit_bytes=60 * 1024 * 1024
        ),
    )(
        source, z_vectors, y_vectors, z_values.reshape(1, -1), y_values.reshape(1, -1),
        x_vectors, x_values,
    )


def fits_whole(n, m, source, z_vectors):
    rows, width = source.shape
    order = z_vectors.shape[0] * n
    return (
        rows == 64 and m == 4 and n <= 8 and n % 2 == 0 and order * order <= 1 << 20
        and z_vectors.shape[1] % 128 == 0 and width % (16 * n * m) == 0
    )


def solution(mesh):
    placed = (P("gz", "col"), P("gz", "col"), P(), P(), P(), P(), P())
    sizes = (mesh.shape["gz"], mesh.shape["col"])

    def body(source, z_vectors, *rest):
        chosen = whole_shards if fits_whole(*sizes, source, z_vectors) else shards
        return chosen(*sizes, source, z_vectors, *rest)

    return jax.shard_map(
        body,
        mesh=mesh, in_specs=placed, out_specs=P("gz", "col"), check_vma=False,
    )
```
